32 devices in a mesh: ens: 4 (over x, core), elem: 8 (over z, y).
Axes of the slice: x: 2, y: 2, z: 4, core: 2. Of those that a mesh axis runs over, the one named last changes fastest.
Arguments:
- scalars: float32 [8, 512, 1024], P('ens', None, 'elem'), parts along dimension 0, may hold values from -6 to 6
- transport: float32 [3, 512, 1024], P(None, None, 'elem'), may hold values from -6 to 6
- mass: float32 [512, 1024], P(None, 'elem'), may hold values from 0.5 to 2
- element_order: int32 [8, 128], P('elem'), may hold values from 0 to 127, each once within a row
Outputs:
- advected: float32 [8, 512, 1024], P('ens', None, 'elem'), parts along dimension 0
The draws below stay inside these ranges and needn't reach their ends.
There are 4 independent parts, one for each index of `ens`. The reference program is written for one: setup_inputs(seed, part) draws one part's arguments, and reference() takes and returns one part's arrays. A program takes and returns all parts, laid end to end along the dimension named above; an argument that names none is the same for every part. Nothing has to cross between parts.
Inputs may be any that keep to these rules, and one draw needn't show every extreme that they name: `element_order`: each row is a permutation of the device's slots.
All inputs are finite; a program needn't handle non-finite values.
Results may differ from the reference program's by a relative error of at most 0.0001.
Values sent between devices are 32-bit elements; how exact they have to be, the bound alone decides.
A program may use at most 64 MiB of HBM per device.

```python
import math
import jax
import jax.numpy as jnp
import numpy as np
from jax import lax

ORDER = 7
NODES = 512
MEMB = 2
SUBSTEPS = 2
EX = 1
EY = 8
EZ = 16
E_DEV = 128
ELEMS = 1024
N_ELEM = 8


def block_levels(own_key, shape, cuts, smallest, largest):
    level, own = 1.0, jax.random.fold_in(own_key, 6)
    for dim, blocks in cuts:
        heights = jnp.exp(jax.random.uniform(jax.random.fold_in(own, dim), (blocks,), jnp.float32, smallest / len(cuts), largest / len(cuts)))
        level = level * jnp.repeat(heights, shape[dim] // blocks).reshape([-1 if axis == dim else 1 for axis in range(len(shape))])
    return level


def bell_draw(own_key, shape, deviation, most, split=(), held_as=jnp.bfloat16):
    result = deviation * jax.random.normal(own_key, shape, jnp.float32)
    if split:
        result = result * block_levels(own_key, shape, split, -0.22, 0.18)
    return jnp.clip(result, -most, most).astype(held_as)


def setup_inputs(seed: int = 0, part: int = 0) -> dict:
    key_list = jax.random.split(jax.random.key(seed), 5)
    part_keys = jax.random.split(jax.random.fold_in(key_list[4], part), 5)
    scalars = bell_draw(part_keys[0], (MEMB, NODES, ELEMS), 1.0, 6.0, ((2, 8),), jnp.float32)
    transport = bell_draw(key_list[1], (3, NODES, ELEMS), 1.0, 6.0, ((2, 8),), jnp.float32)
    mass = jnp.clip(jnp.exp(math.log(2.0) - 1.3862944 * jax.random.uniform(key_list[2], (NODES, ELEMS), jnp.float32) ** block_levels(key_list[2], (NODES, ELEMS), ((1, 8),), -0.2, 0.2)), 0.5, 2.0)
    element_order = jax.vmap(lambda own: jax.random.permutation(own, E_DEV))(jax.random.split(key_list[3], N_ELEM)).reshape((N_ELEM, E_DEV)).astype(jnp.int32)
    return {"scalars": scalars, "transport": transport, "mass": mass, "element_order": element_order}


time_step = 0.015


def legendre_table(points, degree):
    table = np.zeros((points.shape[0], degree + 1))
    table[:, 0] = 1.0
    table[:, 1] = points
    for level in range(2, degree + 1):
        table[:, level] = ((2 * level - 1) * points * table[:, level - 1] - (level - 1) * table[:, level - 2]) / level
    return table


def gll_derivative(degree):
    extent = degree + 1
    points = np.cos(np.pi * np.arange(extent) / degree)
    for sweep in range(60):
        table = legendre_table(points, degree)
        points = points - (points * table[:, degree] - table[:, degree - 1]) / (extent * table[:, degree])
    points = points[::-1].copy()
    values = legendre_table(points, degree)[:, degree]
    matrix = np.zeros((extent, extent))
    for target in range(extent):
        for source in range(extent):
            if target != source:
                matrix[target, source] = values[target] / (values[source] * (points[target] - points[source]))
    matrix[0, 0] = -degree * (degree + 1) / 4.0
    matrix[extent - 1, extent - 1] = degree * (degree + 1) / 4.0
    return matrix


def assemble(field):
    last = ORDER
    upper = field[..., last, :, :, :, :, :] + jnp.roll(field[..., 0, :, :, :, :, :], -1, axis=-3)
    field = field.at[..., last, :, :, :, :, :].set(upper).at[..., 0, :, :, :, :, :].set(jnp.roll(upper, 1, axis=-3))
    upper = field[..., last, :, :, :, :] + jnp.roll(field[..., 0, :, :, :, :], -1, axis=-2)
    field = field.at[..., last, :, :, :, :].set(upper).at[..., 0, :, :, :, :].set(jnp.roll(upper, 1, axis=-2))
    upper = field[..., last, :, :, :] + jnp.roll(field[..., 0, :, :, :], -1, axis=-1)
    field = field.at[..., last, :, :, :].set(upper).at[..., 0, :, :, :].set(jnp.roll(upper, 1, axis=-1))
    return field


def reference(scalars, transport, mass, element_order):
    extent = ORDER + 1
    derivative = jnp.asarray(gll_derivative(ORDER), jnp.float32)
    highest = lax.Precision.HIGHEST
    position = (jnp.arange(N_ELEM, dtype=jnp.int32)[:, None] * E_DEV + element_order.astype(jnp.int32)).reshape(-1)

    def to_brick(values):
        placed = jnp.zeros_like(values).at[..., position].set(values)
        return placed.reshape(values.shape[:-2] + (extent, extent, extent, EX * N_ELEM, EY, EZ))

    field = to_brick(scalars)
    velocity = to_brick(transport)
    weights = to_brick(mass)
    summed = assemble(jnp.concatenate([weights[None] * field, weights[None]], axis=0))
    total_mass = summed[MEMB]
    field = summed[:MEMB] / total_mass

    def tendency(values):
        grad_r = jnp.einsum('ai,...ijkxyz->...ajkxyz', derivative, values, precision=highest)
        grad_s = jnp.einsum('bj,...ijkxyz->...ibkxyz', derivative, values, precision=highest)
        grad_t = jnp.einsum('ck,...ijkxyz->...ijcxyz', derivative, values, precision=highest)
        weighted = velocity[0] * grad_r + velocity[1] * grad_s + velocity[2] * grad_t
        return -assemble(weighted) / total_mass

    for substep in range(SUBSTEPS):
        first_k = tendency(field)
        second_k = tendency(field + 0.5 * time_step * first_k)
        third_k = tendency(field + 0.5 * time_step * second_k)
        fourth_k = tendency(field + time_step * third_k)
        field = field + (time_step / 6.0) * (first_k + 2.0 * second_k + 2.0 * third_k + fourth_k)
    flat = field.reshape(MEMB, NODES, ELEMS)
    return flat[..., position]
```

```python
import functools

import jax
import jax.numpy as jnp
import numpy as np
from jax import lax
from jax.experimental import pallas as pl
from jax.experimental.pallas import tpu as pltpu
from jax.sharding import PartitionSpec as P

ORDER = 7
SUBSTEPS = 2
EX = 1
EY = 8
EZ = 16
EXTENT = ORDER + 1
PLANE = EXTENT * EXTENT
NODES = EXTENT * PLANE
MESH = pl.DeviceIdType.MESH


time_step = 0.015


def legendre_table(points, degree):
    table = np.zeros((points.shape[0], degree + 1))
    table[:, 0] = 1.0
    table[:, 1] = points
    for level in range(2, degree + 1):
        table[:, level] = (
            (2 * level - 1) * points * table[:, level - 1] - (level - 1) * table[:, level - 2]
        ) / level
    return table


def gll_derivative(degree):
    extent = degree + 1
    points = np.cos(np.pi * np.arange(extent) / degree)
    for sweep in range(60):
        table = legendre_table(points, degree)
        points = points - (points * table[:, degree] - table[:, degree - 1]) / (
            extent * table[:, degree]
        )
    points = points[::-1].copy()
    values = legendre_table(points, degree)[:, degree]
    matrix = np.zeros((extent, extent))
    for target in range(extent):
        for source in range(extent):
            if target != source:
                matrix[target, source] = values[target] / (
                    values[source] * (points[target] - points[source])
                )
    matrix[0, 0] = -degree * (degree + 1) / 4.0
    matrix[extent - 1, extent - 1] = degree * (degree + 1) / 4.0
    return matrix


def split_matrix():
    derivative = gll_derivative(ORDER).astype(np.float32)
    eye = np.eye(EXTENT, dtype=np.float32)
    full = np.concatenate([np.kron(derivative, eye), np.kron(eye, derivative)], axis=0)
    high = full.astype(jnp.bfloat16)
    low = (full - high.astype(np.float32)).astype(jnp.bfloat16)
    return np.concatenate([high, high, low], axis=1)


def halves(values):
    high = values.astype(jnp.bfloat16)
    low = (values - high.astype(jnp.float32)).astype(jnp.bfloat16)
    return high, low


def lane_forward(values, stride, length):
    total = values.shape[-1]
    near = pltpu.roll(values, total - stride, 1)
    if stride * length == total:
        return near
    coords = lax.broadcasted_iota(jnp.int32, values.shape, 1) // stride % length
    return jnp.where(coords < length - 1, near, pltpu.roll(values, stride * (length - 1), 1))


def lane_backward(values, stride, length):
    total = values.shape[-1]
    near = pltpu.roll(values, stride, 1)
    if stride * length == total:
        return near
    coords = lax.broadcasted_iota(jnp.int32, values.shape, 1) // stride % length
    return jnp.where(coords > 0, near, pltpu.roll(values, total - stride * (length - 1), 1))


def store_assembled(ref, row, values):
    low, high = values[:EXTENT], values[PLANE - EXTENT :]
    ref[row : row + EXTENT] = low + lane_backward(high, EZ, EY)
    ref[row + EXTENT : row + PLANE - EXTENT] = values[EXTENT : PLANE - EXTENT]
    ref[row + PLANE - EXTENT : row + PLANE] = high + lane_forward(low, EZ, EY)
    first = pl.ds(row, EXTENT, stride=EXTENT)
    last = pl.ds(row + ORDER, EXTENT, stride=EXTENT)
    k_low = ref[first, :]
    k_high = ref[last, :]
    ref[first, :] = k_low + lane_backward(k_high, 1, EZ)
    ref[last, :] = k_high + lane_forward(k_low, 1, EZ)


def kernel(
    count, members, scalars, transport, mass, order, matrix, out,
    speed, current, base, total, work, inverse, send, recv, send_sem, recv_sem,
):
    me = lax.axis_index("elem")
    right, left = lax.rem(me + 1, count), lax.rem(me + count - 1, count)
    barrier = pltpu.get_barrier_semaphore()
    for neighbour in (left, right):
        pl.semaphore_signal(barrier, inc=1, device_id={"elem": neighbour}, device_id_type=MESH)
    pl.semaphore_wait(barrier, 2)

    elements = order.shape[-1]
    lanes = lax.broadcasted_iota(jnp.int32, (elements, elements), 0)
    chosen = jnp.where(order[...] == lanes, 1.0, 0.0).astype(jnp.bfloat16)
    to_brick_matrix = jnp.concatenate([chosen, chosen], axis=1)
    to_slot_matrix = jnp.concatenate([chosen, chosen], axis=0)

    def to_brick(values):
        return lax.dot_general(
            jnp.concatenate(halves(values), axis=1),
            to_brick_matrix,
            (((1,), (1,)), ((), ())),
            preferred_element_type=jnp.float32,
        )

    def exchange(slot, rows):
        copies = []
        for side, target in ((0, right), (1, left)):
            copy = pltpu.make_async_remote_copy(
                src_ref=send.at[slot, side, pl.ds(0, rows)],
                dst_ref=recv.at[slot, side, pl.ds(0, rows)],
                send_sem=send_sem.at[slot, side],
                recv_sem=recv_sem.at[slot, side],
                device_id={"elem": target},
                device_id_type=MESH,
            )
            copy.start()
            copies.append(copy)
        return copies

    brick_mass = {}
    for i in (0, ORDER, *range(1, ORDER)):
        rows = slice(i * PLANE, (i + 1) * PLANE)
        weight = to_brick(mass[rows, :])
        for m in range(members + 1):
            value = weight if m == members else weight * to_brick(scalars[m, rows, :])
            if i in (0, ORDER):
                store_assembled(send.at[1, 0 if i == ORDER else 1], m * PLANE, value)
            else:
                store_assembled(work, (m * EXTENT + i) * PLANE, value)
        if i == ORDER:
            copies = exchange(1, (members + 1) * PLANE)
    for r in range(3):
        for i in range(EXTENT):
            rows = slice(i * PLANE, (i + 1) * PLANE)
            speed[r, rows, :] = to_brick(transport[r, rows, :])
    for copy in copies:
        copy.wait()
    for i in range(EXTENT):
        rows = slice(i * PLANE, (i + 1) * PLANE)

        def summed(m):
            if i == 0:
                part = slice(m * PLANE, (m + 1) * PLANE)
                return send[1, 1, part, :] + recv[1, 0, part, :]
            if i == ORDER:
                part = slice(m * PLANE, (m + 1) * PLANE)
                return send[1, 0, part, :] + recv[1, 1, part, :]
            return work[(m * EXTENT + i) * PLANE : (m * EXTENT + i + 1) * PLANE, :]

        scale = 1.0 / summed(members)
        for r in range(3):
            speed[r, rows, :] = -speed[r, rows, :] * scale
        for m in range(members):
            part = slice((m * EXTENT + i) * PLANE, (m * EXTENT + i + 1) * PLANE)
            value = summed(m) * scale
            current[0, part, :] = value
            base[part, :] = value
            total[part, :] = value

    derivative = gll_derivative(ORDER)
    half = EXTENT // 2

    def stage(index, carry):
        slot = lax.rem(index, 2)
        step = lax.rem(index, 4)
        last = step == 3
        weight = jnp.where(jnp.logical_or(step == 0, last), time_step / 6.0, time_step / 3.0)
        reach = jnp.where(step == 2, time_step, 0.5 * time_step)

        def plane(m, i):
            return current[slot, (m * EXTENT + i) * PLANE : (m * EXTENT + i + 1) * PLANE, :]

        def in_plane(i):
            stacked = []
            for m in range(members):
                high, low = halves(plane(m, i))
                stacked.append(jnp.concatenate([high, low, high], axis=0))
            return jnp.dot(
                matrix[...],
                jnp.concatenate(stacked, axis=1),
                preferred_element_type=jnp.float32,
            )

        def pair(a):
            inside = {a: in_plane(a), ORDER - a: in_plane(ORDER - a)}
            for m in range(members):
                even = odd = None
                for i in range(half):
                    near, far = plane(m, i), plane(m, ORDER - i)
                    plus = float(derivative[a, i] + derivative[a, ORDER - i]) * 0.5
                    minus = float(derivative[a, i] - derivative[a, ORDER - i]) * 0.5
                    even_term = plus * (near + far)
                    odd_term = minus * (near - far)
                    even = even_term if even is None else even + even_term
                    odd = odd_term if odd is None else odd + odd_term
                for i, across in ((a, odd + even), (ORDER - a, odd - even)):
                    rows = slice(i * PLANE, (i + 1) * PLANE)
                    columns = slice(m * elements, (m + 1) * elements)
                    yield m, i, (
                        speed[0, rows, :] * across
                        + speed[1, rows, :] * inside[i][:PLANE, columns]
                        + speed[2, rows, :] * inside[i][PLANE:, columns]
                    )

        def advance(m, i, tendency):
            part = slice((m * EXTENT + i) * PLANE, (m * EXTENT + i + 1) * PLANE)
            start = base[part, :]
            summed = total[part, :] + weight * tendency
            total[part, :] = summed
            current[1 - slot, part, :] = jnp.where(last, summed, start + reach * tendency)
            base[part, :] = jnp.where(last, summed, start)

        for m, i, value in pair(0):
            store_assembled(send.at[slot, 0 if i == ORDER else 1], m * PLANE, value)
        copies = exchange(slot, members * PLANE)
        for a in range(1, half):
            for m, i, value in pair(a):
                store_assembled(work, (m * EXTENT + i) * PLANE, value)
            for m in range(members):
                for i in (a, ORDER - a):
                    advance(m, i, work[(m * EXTENT + i) * PLANE : (m * EXTENT + i + 1) * PLANE, :])
        for copy in copies:
            copy.wait()
        for m in range(members):
            part = slice(m * PLANE, (m + 1) * PLANE)
            advance(m, 0, send[slot, 1, part, :] + recv[slot, 0, part, :])
            advance(m, ORDER, send[slot, 0, part, :] + recv[slot, 1, part, :])
        return carry

    lax.fori_loop(0, 4 * SUBSTEPS, stage, 0)
    for m in range(members):
        out[m, :, :] = jnp.dot(
            jnp.concatenate(halves(total[m * NODES : (m + 1) * NODES, :]), axis=1),
            to_slot_matrix,
            preferred_element_type=jnp.float32,
        )


def per_device(scalars, transport, mass, element_order):
    members, nodes, elements = scalars.shape
    count = lax.axis_size("elem")
    whole = pl.BlockSpec(memory_space=pltpu.VMEM)
    return pl.pallas_call(
        functools.partial(kernel, count, members),
        out_shape=jax.ShapeDtypeStruct(scalars.shape, jnp.float32),
        in_specs=[whole] * 5,
        out_specs=whole,
        scratch_shapes=[
            pltpu.VMEM((3, nodes, elements), jnp.float32),
            pltpu.VMEM((2, members * nodes, elements), jnp.float32),
            pltpu.VMEM((members * nodes, elements), jnp.float32),
            pltpu.VMEM((members * nodes, elements), jnp.float32),
            pltpu.VMEM(((members + 1) * nodes, elements), jnp.float32),
            pltpu.VMEM((8, elements), jnp.float32),
            pltpu.VMEM((2, 2, (members + 1) * PLANE, elements), jnp.float32),
            pltpu.VMEM((2, 2, (members + 1) * PLANE, elements), jnp.float32),
            pltpu.SemaphoreType.DMA((2, 2)),
            pltpu.SemaphoreType.DMA((2, 2)),
        ],
        compiler_params=pltpu.CompilerParams(collective_id=0, has_side_effects=True),
    )(scalars, transport, mass, element_order, jnp.asarray(split_matrix()))


def solution(mesh):
    in_specs = (P("ens", None, "elem"), P(None, None, "elem"), P(None, "elem"), P("elem", None))
    out_specs = P("ens", None, "elem")
    return jax.shard_map(
        per_device, mesh=mesh, in_specs=in_specs, out_specs=out_specs, check_vma=False
    )
```

```python
import functools

import jax
import jax.numpy as jnp
import numpy as np
from jax import lax
from jax.experimental import pallas as pl
from jax.experimental.pallas import tpu as pltpu
from jax.sharding import PartitionSpec as P

ORDER = 7
SUBSTEPS = 2
EX = 1
EY = 8
EZ = 16
EXTENT = ORDER + 1
PLANE = EXTENT * EXTENT
NODES = EXTENT * PLANE
MESH = pl.DeviceIdType.MESH


time_step = 0.015


def legendre_table(points, degree):
    table = np.zeros((points.shape[0], degree + 1))
    table[:, 0] = 1.0
    table[:, 1] = points
    for level in range(2, degree + 1):
        table[:, level] = (
            (2 * level - 1) * points * table[:, level - 1] - (level - 1) * table[:, level - 2]
        ) / level
    return table


def gll_derivative(degree):
    extent = degree + 1
    points = np.cos(np.pi * np.arange(extent) / degree)
    for sweep in range(60):
        table = legendre_table(points, degree)
        points = points - (points * table[:, degree] - table[:, degree - 1]) / (
            extent * table[:, degree]
        )
    points = points[::-1].copy()
    values = legendre_table(points, degree)[:, degree]
    matrix = np.zeros((extent, extent))
    for target in range(extent):
        for source in range(extent):
            if target != source:
                matrix[target, source] = values[target] / (
                    values[source] * (points[target] - points[source])
                )
    matrix[0, 0] = -degree * (degree + 1) / 4.0
    matrix[extent - 1, extent - 1] = degree * (degree + 1) / 4.0
    return matrix


def split_matrix():
    derivative = gll_derivative(ORDER).astype(np.float32)
    eye = np.eye(EXTENT, dtype=np.float32)
    full = np.concatenate([np.kron(derivative, eye), np.kron(eye, derivative)], axis=0)
    high = full.astype(jnp.bfloat16)
    low = (full - high.astype(np.float32)).astype(jnp.bfloat16)
    return np.concatenate([high, high, low], axis=1)


def halves(values):
    high = values.astype(jnp.bfloat16)
    low = (values - high.astype(jnp.float32)).astype(jnp.bfloat16)
    return high, low


def lane_forward(values, stride, length):
    total = values.shape[-1]
    near = pltpu.roll(values, total - stride, 1)
    if stride * length == total:
        return near
    coords = lax.broadcasted_iota(jnp.int32, values.shape, 1) // stride % length
    return jnp.where(coords < length - 1, near, pltpu.roll(values, stride * (length - 1), 1))


def lane_backward(values, stride, length):
    total = values.shape[-1]
    near = pltpu.roll(values, stride, 1)
    if stride * length == total:
        return near
    coords = lax.broadcasted_iota(jnp.int32, values.shape, 1) // stride % length
    return jnp.where(coords > 0, near, pltpu.roll(values, total - stride * (length - 1), 1))


def store_assembled(ref, row, values):
    low, high = values[:EXTENT], values[PLANE - EXTENT :]
    ref[row : row + EXTENT] = low + lane_backward(high, EZ, EY)
    ref[row + EXTENT : row + PLANE - EXTENT] = values[EXTENT : PLANE - EXTENT]
    ref[row + PLANE - EXTENT : row + PLANE] = high + lane_forward(low, EZ, EY)
    first = pl.ds(row, EXTENT, stride=EXTENT)
    last = pl.ds(row + ORDER, EXTENT, stride=EXTENT)
    k_low = ref[first, :]
    k_high = ref[last, :]
    ref[first, :] = k_low + lane_backward(k_high, 1, EZ)
    ref[last, :] = k_high + lane_forward(k_low, 1, EZ)


def store_lower(ref, row, values):
    low, high = values[:EXTENT], values[PLANE - EXTENT :]
    ref[row : row + EXTENT] = low + lane_backward(high, EZ, EY)
    ref[row + EXTENT : row + PLANE] = values[EXTENT:]
    first = pl.ds(row, EXTENT, stride=EXTENT)
    k_high = ref[pl.ds(row + ORDER, EXTENT, stride=EXTENT), :]
    ref[first, :] = ref[first, :] + lane_backward(k_high, 1, EZ)


def pack(source, row, target):
    for j in range(ORDER):
        target[j * ORDER : j * ORDER + EXTENT] = source[row + j * EXTENT : row + (j + 1) * EXTENT]


def add_packed(ref, row, packed):
    for j in range(ORDER):
        part = slice(row + j * EXTENT, row + (j + 1) * EXTENT)
        ref[part] = ref[part] + packed[j * ORDER : j * ORDER + EXTENT]
    k_low = ref[pl.ds(row, EXTENT, stride=EXTENT), :]
    ref[pl.ds(row + ORDER, EXTENT, stride=EXTENT), :] = lane_forward(k_low, 1, EZ)
    ref[row + PLANE - EXTENT : row + PLANE] = lane_forward(ref[row : row + EXTENT], EZ, EY)


def kernel(
    count, members, scalars, transport, mass, order, matrix, out,
    speed, current, base, total, work, send, recv, send_sem, recv_sem,
):
    me = lax.axis_index("elem")
    right, left = lax.rem(me + 1, count), lax.rem(me + count - 1, count)
    barrier = pltpu.get_barrier_semaphore()
    for neighbour in (left, right):
        pl.semaphore_signal(barrier, inc=1, device_id={"elem": neighbour}, device_id_type=MESH)

    elements = order.shape[-1]
    lanes = lax.broadcasted_iota(jnp.int32, (elements, elements), 0)
    chosen = jnp.where(order[...] == lanes, 1.0, 0.0).astype(jnp.bfloat16)
    to_brick_matrix = jnp.concatenate([chosen, chosen], axis=1)
    to_slot_matrix = jnp.concatenate([chosen, chosen], axis=0)

    def to_brick(values):
        return lax.dot_general(
            jnp.concatenate(halves(values), axis=1),
            to_brick_matrix,
            (((1,), (1,)), ((), ())),
            preferred_element_type=jnp.float32,
        )

    first_side = 1 - lax.rem(me, 2)
    sides = (first_side, 1 - first_side)

    def copies_of(slot, m):
        copies = []
        for side in sides:
            copies.append(
                pltpu.make_async_remote_copy(
                    src_ref=send.at[slot, m, side, pl.ds(0, ORDER * ORDER)],
                    dst_ref=recv.at[slot, m, side, pl.ds(0, ORDER * ORDER)],
                    send_sem=send_sem.at[slot, m, side],
                    recv_sem=recv_sem.at[slot, m, side],
                    device_id={"elem": side * left + (1 - side) * right},
                    device_id_type=MESH,
                )
            )
        return copies

    def start(slot, m):
        for copy in copies_of(slot, m):
            copy.start()

    def finish(slot, m):
        for copy in copies_of(slot, m):
            copy.wait()

    def row_of(m, i):
        return (m * EXTENT + i) * PLANE

    def rows_of(m, i):
        return slice(row_of(m, i), row_of(m, i) + PLANE)

    def plane_rows(i):
        return slice(i * PLANE, (i + 1) * PLANE)

    def put_face(slot, m, i, value):
        store_lower(work, row_of(m, i), value)
        pack(work, row_of(m, i), send.at[slot, m, 0 if i == ORDER else 1])

    def take_faces(slot, m):
        finish(slot, m)
        add_packed(work, row_of(m, 0), recv.at[slot, m, 0])
        add_packed(work, row_of(m, ORDER), recv.at[slot, m, 1])

    weights = {}
    for i in (0, ORDER):
        weights[i] = to_brick(mass[plane_rows(i), :])
        put_face(1, members, i, weights[i])
    pl.semaphore_wait(barrier, 2)
    start(1, members)
    for m in range(members):
        for i in (0, ORDER):
            put_face(1, m, i, weights[i] * to_brick(scalars[m, plane_rows(i), :]))
        start(1, m)
    for i in range(1, ORDER):
        weight = to_brick(mass[plane_rows(i), :])
        store_assembled(work, row_of(members, i), weight)
        for m in range(members):
            store_assembled(work, row_of(m, i), weight * to_brick(scalars[m, plane_rows(i), :]))
    for r in range(3):
        for i in range(EXTENT):
            speed[r, plane_rows(i), :] = to_brick(transport[r, plane_rows(i), :])

    def begin(m, i):
        value = work[rows_of(m, i), :] * work[rows_of(members, i), :]
        current[0, rows_of(m, i), :] = value
        base[rows_of(m, i), :] = value
        total[rows_of(m, i), :] = value

    def scale(i):
        inverse = 1.0 / work[rows_of(members, i), :]
        work[rows_of(members, i), :] = inverse
        for r in range(3):
            speed[r, plane_rows(i), :] = -speed[r, plane_rows(i), :] * inverse

    for i in range(1, ORDER):
        scale(i)
        for m in range(members):
            begin(m, i)
    take_faces(1, members)
    scale(0)
    scale(ORDER)

    derivative = gll_derivative(ORDER)
    half = EXTENT // 2

    def pair(slot, m, a):
        def plane(i):
            return current[slot, rows_of(m, i), :]

        even = odd = None
        for i in range(half):
            near, far = plane(i), plane(ORDER - i)
            plus = float(derivative[a, i] + derivative[a, ORDER - i]) * 0.5
            minus = float(derivative[a, i] - derivative[a, ORDER - i]) * 0.5
            even_term = plus * (near + far)
            odd_term = minus * (near - far)
            even = even_term if even is None else even + even_term
            odd = odd_term if odd is None else odd + odd_term
        stacked = []
        for i in (a, ORDER - a):
            high, low = halves(plane(i))
            stacked.append(jnp.concatenate([high, low, high], axis=0))
        inside = jnp.dot(
            matrix[...],
            jnp.concatenate(stacked, axis=1),
            preferred_element_type=jnp.float32,
        )
        for place, (i, across) in enumerate(((a, odd + even), (ORDER - a, odd - even))):
            columns = slice(place * elements, (place + 1) * elements)
            yield i, (
                speed[0, plane_rows(i), :] * across
                + speed[1, plane_rows(i), :] * inside[:PLANE, columns]
                + speed[2, plane_rows(i), :] * inside[PLANE:, columns]
            )

    def advance(index, m, i):
        step = lax.rem(index, 4)
        last = step == 3
        weight = jnp.where(jnp.logical_or(step == 0, last), time_step / 6.0, time_step / 3.0)
        reach = jnp.where(step == 2, time_step, 0.5 * time_step)
        tendency = work[rows_of(m, i), :]
        origin = base[rows_of(m, i), :]
        summed = total[rows_of(m, i), :] + weight * tendency
        total[rows_of(m, i), :] = summed
        current[1 - lax.rem(index, 2), rows_of(m, i), :] = jnp.where(
            last, summed, origin + reach * tendency
        )
        base[rows_of(m, i), :] = jnp.where(last, summed, origin)

    def close(index, m):
        take_faces(lax.rem(index, 2), m)
        advance(index, m, 0)
        advance(index, m, ORDER)

    def open_faces(index, m):
        slot = lax.rem(index, 2)
        for i, value in pair(slot, m, 0):
            put_face(slot, m, i, value)
        start(slot, m)

    def interior(index):
        for m in range(members):
            for a in range(1, half):
                for i, value in pair(lax.rem(index, 2), m, a):
                    store_assembled(work, row_of(m, i), value)
                    advance(index, m, i)

    for m in range(members):
        take_faces(1, m)
        begin(m, 0)
        begin(m, ORDER)
        open_faces(0, m)
    interior(0)

    def stage(index, carry):
        for m in range(members):
            close(index - 1, m)
            open_faces(index, m)
        interior(index)
        return carry

    final = 4 * SUBSTEPS - 1
    lax.fori_loop(1, final + 1, stage, 0)
    for m in range(members):
        close(final, m)
        out[m, :, :] = jnp.dot(
            jnp.concatenate(halves(total[m * NODES : (m + 1) * NODES, :]), axis=1),
            to_slot_matrix,
            preferred_element_type=jnp.float32,
        )


def per_device(scalars, transport, mass, element_order):
    members, nodes, elements = scalars.shape
    count = lax.axis_size("elem")
    whole = pl.BlockSpec(memory_space=pltpu.VMEM)
    return pl.pallas_call(
        functools.partial(kernel, count, members),
        out_shape=jax.ShapeDtypeStruct(scalars.shape, jnp.float32),
        in_specs=[whole] * 5,
        out_specs=whole,
        scratch_shapes=[
            pltpu.VMEM((3, nodes, elements), jnp.float32),
            pltpu.VMEM((2, members * nodes, elements), jnp.float32),
            pltpu.VMEM((members * nodes, elements), jnp.float32),
            pltpu.VMEM((members * nodes, elements), jnp.float32),
            pltpu.VMEM(((members + 1) * nodes, elements), jnp.float32),
            pltpu.VMEM((2, members + 1, 2, PLANE - EXTENT, elements), jnp.float32),
            pltpu.VMEM((2, members + 1, 2, PLANE - EXTENT, elements), jnp.float32),
            pltpu.SemaphoreType.DMA((2, members + 1, 2)),
            pltpu.SemaphoreType.DMA((2, members + 1, 2)),
        ],
        compiler_params=pltpu.CompilerParams(collective_id=0, has_side_effects=True),
    )(scalars, transport, mass, element_order, jnp.asarray(split_matrix()))


def solution(mesh):
    in_specs = (P("ens", None, "elem"), P(None, None, "elem"), P(None, "elem"), P("elem", None))
    out_specs = P("ens", None, "elem")
    return jax.shard_map(
        per_device, mesh=mesh, in_specs=in_specs, out_specs=out_specs, check_vma=False
    )
```

```python
import functools

import jax
import jax.numpy as jnp
import numpy as np
from jax import lax
from jax.experimental import pallas as pl
from jax.experimental.pallas import tpu as pltpu
from jax.sharding import PartitionSpec as P

ORDER = 7
SUBSTEPS = 2
EX = 1
EY = 8
EZ = 16
EXTENT = ORDER + 1
PLANE = EXTENT * EXTENT
NODES = EXTENT * PLANE
MESH = pl.DeviceIdType.MESH


time_step = 0.015


def legendre_table(points, degree):
    table = np.zeros((points.shape[0], degree + 1))
    table[:, 0] = 1.0
    table[:, 1] = points
    for level in range(2, degree + 1):
        table[:, level] = (
            (2 * level - 1) * points * table[:, level - 1] - (level - 1) * table[:, level - 2]
        ) / level
    return table


def gll_derivative(degree):
    extent = degree + 1
    points = np.cos(np.pi * np.arange(extent) / degree)
    for sweep in range(60):
        table = legendre_table(points, degree)
        points = points - (points * table[:, degree] - table[:, degree - 1]) / (
            extent * table[:, degree]
        )
    points = points[::-1].copy()
    values = legendre_table(points, degree)[:, degree]
    matrix = np.zeros((extent, extent))
    for target in range(extent):
        for source in range(extent):
            if target != source:
                matrix[target, source] = values[target] / (
                    values[source] * (points[target] - points[source])
                )
    matrix[0, 0] = -degree * (degree + 1) / 4.0
    matrix[extent - 1, extent - 1] = degree * (degree + 1) / 4.0
    return matrix


def split_matrix():
    derivative = gll_derivative(ORDER).astype(np.float32)
    eye = np.eye(EXTENT, dtype=np.float32)
    full = np.concatenate([np.kron(derivative, eye), np.kron(eye, derivative)], axis=0)
    high = full.astype(jnp.bfloat16)
    low = (full - high.astype(np.float32)).astype(jnp.bfloat16)
    return np.concatenate([high, high, low], axis=1)


def halves(values):
    high = values.astype(jnp.bfloat16)
    low = (values - high.astype(jnp.float32)).astype(jnp.bfloat16)
    return high, low


def lane_forward(values, stride, length):
    total = values.shape[-1]
    near = pltpu.roll(values, total - stride, 1)
    if stride * length == total:
        return near
    coords = lax.broadcasted_iota(jnp.int32, values.shape, 1) // stride % length
    return jnp.where(coords < length - 1, near, pltpu.roll(values, stride * (length - 1), 1))


def lane_backward(values, stride, length):
    total = values.shape[-1]
    near = pltpu.roll(values, stride, 1)
    if stride * length == total:
        return near
    coords = lax.broadcasted_iota(jnp.int32, values.shape, 1) // stride % length
    return jnp.where(coords > 0, near, pltpu.roll(values, total - stride * (length - 1), 1))


def store_assembled(ref, row, values):
    low, high = values[:EXTENT], values[PLANE - EXTENT :]
    ref[row : row + EXTENT] = low + lane_backward(high, EZ, EY)
    ref[row + EXTENT : row + PLANE - EXTENT] = values[EXTENT : PLANE - EXTENT]
    ref[row + PLANE - EXTENT : row + PLANE] = high + lane_forward(low, EZ, EY)
    first = pl.ds(row, EXTENT, stride=EXTENT)
    last = pl.ds(row + ORDER, EXTENT, stride=EXTENT)
    k_low = ref[first, :]
    k_high = ref[last, :]
    ref[first, :] = k_low + lane_backward(k_high, 1, EZ)
    ref[last, :] = k_high + lane_forward(k_low, 1, EZ)


def store_lower(ref, row, values):
    low, high = values[:EXTENT], values[PLANE - EXTENT :]
    ref[row : row + EXTENT] = low + lane_backward(high, EZ, EY)
    ref[row + EXTENT : row + PLANE] = values[EXTENT:]
    first = pl.ds(row, EXTENT, stride=EXTENT)
    k_high = ref[pl.ds(row + ORDER, EXTENT, stride=EXTENT), :]
    ref[first, :] = ref[first, :] + lane_backward(k_high, 1, EZ)


def pack(source, row, target):
    for j in range(ORDER):
        target[j * ORDER : j * ORDER + EXTENT] = source[row + j * EXTENT : row + (j + 1) * EXTENT]


def add_packed(ref, row, packed):
    for j in range(ORDER):
        part = slice(row + j * EXTENT, row + (j + 1) * EXTENT)
        ref[part] = ref[part] + packed[j * ORDER : j * ORDER + EXTENT]
    k_low = ref[pl.ds(row, EXTENT, stride=EXTENT), :]
    ref[pl.ds(row + ORDER, EXTENT, stride=EXTENT), :] = lane_forward(k_low, 1, EZ)
    ref[row + PLANE - EXTENT : row + PLANE] = lane_forward(ref[row : row + EXTENT], EZ, EY)


def kernel(
    count, members, scalars_in, transport_in, mass_in, order, matrix, total,
    scalars, transport, mass, speed, current, base, work, send, recv, load_sem, send_sem, recv_sem,
):
    loads = [
        pltpu.make_async_copy(source, target, load_sem.at[place])
        for place, (source, target) in enumerate(
            ((mass_in, mass), (scalars_in, scalars), (transport_in, transport))
        )
    ]
    for load in loads:
        load.start()
    me = lax.axis_index("elem")
    right, left = lax.rem(me + 1, count), lax.rem(me + count - 1, count)
    barrier = pltpu.get_barrier_semaphore()
    for neighbour in (left, right):
        pl.semaphore_signal(barrier, inc=1, device_id={"elem": neighbour}, device_id_type=MESH)

    elements = order.shape[-1]
    lanes = lax.broadcasted_iota(jnp.int32, (elements, elements), 0)
    chosen = jnp.where(order[...] == lanes, 1.0, 0.0).astype(jnp.bfloat16)
    to_brick_matrix = jnp.concatenate([chosen, chosen], axis=1)

    def to_brick(values):
        return lax.dot_general(
            jnp.concatenate(halves(values), axis=1),
            to_brick_matrix,
            (((1,), (1,)), ((), ())),
            preferred_element_type=jnp.float32,
        )

    first_side = 1 - lax.rem(me, 2)
    sides = (first_side, 1 - first_side)

    def copies_of(slot, m):
        copies = []
        for side in sides:
            copies.append(
                pltpu.make_async_remote_copy(
                    src_ref=send.at[slot, m, side, pl.ds(0, ORDER * ORDER)],
                    dst_ref=recv.at[slot, m, side, pl.ds(0, ORDER * ORDER)],
                    send_sem=send_sem.at[slot, m, side],
                    recv_sem=recv_sem.at[slot, m, side],
                    device_id={"elem": side * left + (1 - side) * right},
                    device_id_type=MESH,
                )
            )
        return copies

    def start(slot, m):
        for copy in copies_of(slot, m):
            copy.start()

    def finish(slot, m):
        for copy in copies_of(slot, m):
            copy.wait()

    def row_of(m, i):
        return (m * EXTENT + i) * PLANE

    def rows_of(m, i):
        return slice(row_of(m, i), row_of(m, i) + PLANE)

    def plane_rows(i):
        return slice(i * PLANE, (i + 1) * PLANE)

    def put_face(slot, m, i, value):
        store_lower(work, row_of(m, i), value)
        pack(work, row_of(m, i), send.at[slot, m, 0 if i == ORDER else 1])

    def take_faces(slot, m):
        finish(slot, m)
        add_packed(work, row_of(m, 0), recv.at[slot, m, 0])
        add_packed(work, row_of(m, ORDER), recv.at[slot, m, 1])

    loads[0].wait()
    weights = {}
    for i in (0, ORDER):
        weights[i] = to_brick(mass[plane_rows(i), :])
        put_face(1, members, i, weights[i])
    pl.semaphore_wait(barrier, 2)
    start(1, members)
    loads[1].wait()
    for m in range(members):
        for i in (0, ORDER):
            put_face(1, m, i, weights[i] * to_brick(scalars[m, plane_rows(i), :]))
        start(1, m)
    for i in range(1, ORDER):
        weight = to_brick(mass[plane_rows(i), :])
        store_assembled(work, row_of(members, i), weight)
        for m in range(members):
            store_assembled(work, row_of(m, i), weight * to_brick(scalars[m, plane_rows(i), :]))
    loads[2].wait()
    for r in range(3):
        for i in range(EXTENT):
            speed[r, plane_rows(i), :] = to_brick(transport[r, plane_rows(i), :])

    def begin(m, i):
        value = work[rows_of(m, i), :] * work[rows_of(members, i), :]
        current[0, rows_of(m, i), :] = value
        base[rows_of(m, i), :] = value
        total[rows_of(m, i), :] = value

    def scale(i):
        inverse = 1.0 / work[rows_of(members, i), :]
        work[rows_of(members, i), :] = inverse
        for r in range(3):
            speed[r, plane_rows(i), :] = -speed[r, plane_rows(i), :] * inverse

    for i in range(1, ORDER):
        scale(i)
        for m in range(members):
            begin(m, i)
    take_faces(1, members)
    scale(0)
    scale(ORDER)

    derivative = gll_derivative(ORDER)
    half = EXTENT // 2

    def pair(slot, m, a):
        def plane(i):
            return current[slot, rows_of(m, i), :]

        even = odd = None
        for i in range(half):
            near, far = plane(i), plane(ORDER - i)
            plus = float(derivative[a, i] + derivative[a, ORDER - i]) * 0.5
            minus = float(derivative[a, i] - derivative[a, ORDER - i]) * 0.5
            even_term = plus * (near + far)
            odd_term = minus * (near - far)
            even = even_term if even is None else even + even_term
            odd = odd_term if odd is None else odd + odd_term
        stacked = []
        for i in (a, ORDER - a):
            high, low = halves(plane(i))
            stacked.append(jnp.concatenate([high, low, high], axis=0))
        inside = jnp.dot(
            matrix[...],
            jnp.concatenate(stacked, axis=1),
            preferred_element_type=jnp.float32,
        )
        for place, (i, across) in enumerate(((a, odd + even), (ORDER - a, odd - even))):
            columns = slice(place * elements, (place + 1) * elements)
            yield i, (
                speed[0, plane_rows(i), :] * across
                + speed[1, plane_rows(i), :] * inside[:PLANE, columns]
                + speed[2, plane_rows(i), :] * inside[PLANE:, columns]
            )

    def advance(index, m, i):
        step = lax.rem(index, 4)
        last = step == 3
        weight = jnp.where(jnp.logical_or(step == 0, last), time_step / 6.0, time_step / 3.0)
        reach = jnp.where(step == 2, time_step, 0.5 * time_step)
        tendency = work[rows_of(m, i), :]
        origin = base[rows_of(m, i), :]
        summed = total[rows_of(m, i), :] + weight * tendency
        total[rows_of(m, i), :] = summed
        current[1 - lax.rem(index, 2), rows_of(m, i), :] = jnp.where(
            last, summed, origin + reach * tendency
        )
        base[rows_of(m, i), :] = jnp.where(last, summed, origin)

    def close(index, m):
        take_faces(lax.rem(index, 2), m)
        advance(index, m, 0)
        advance(index, m, ORDER)

    def open_faces(index, m):
        slot = lax.rem(index, 2)
        for i, value in pair(slot, m, 0):
            put_face(slot, m, i, value)
        start(slot, m)

    def interior(index):
        for m in range(members):
            for a in range(1, half):
                for i, value in pair(lax.rem(index, 2), m, a):
                    store_assembled(work, row_of(m, i), value)
                    advance(index, m, i)

    for m in range(members):
        take_faces(1, m)
        begin(m, 0)
        begin(m, ORDER)
        open_faces(0, m)
    interior(0)

    def stage(index, carry):
        for m in range(members):
            close(index - 1, m)
            open_faces(index, m)
        interior(index)
        return carry

    final = 4 * SUBSTEPS - 1
    lax.fori_loop(1, final + 1, stage, 0)
    for m in range(members):
        close(final, m)


def slot_kernel(order, values, out):
    elements = order.shape[-1]
    lanes = lax.broadcasted_iota(jnp.int32, (elements, elements), 0)
    chosen = jnp.where(order[...] == lanes, 1.0, 0.0).astype(jnp.bfloat16)
    out[...] = jnp.dot(
        jnp.concatenate(halves(values[...]), axis=1),
        jnp.concatenate([chosen, chosen], axis=0),
        preferred_element_type=jnp.float32,
    )


def per_device(scalars, transport, mass, element_order):
    members, nodes, elements = scalars.shape
    count = lax.axis_size("elem")
    whole = pl.BlockSpec(memory_space=pltpu.VMEM)
    rows = members * nodes
    outside = pl.BlockSpec(memory_space=pltpu.HBM)
    final = pl.pallas_call(
        functools.partial(kernel, count, members),
        out_shape=jax.ShapeDtypeStruct((rows, elements), jnp.float32),
        in_specs=[outside] * 3 + [whole] * 2,
        out_specs=whole,
        scratch_shapes=[
            pltpu.VMEM(scalars.shape, jnp.float32),
            pltpu.VMEM(transport.shape, jnp.float32),
            pltpu.VMEM(mass.shape, jnp.float32),
            pltpu.VMEM((3, nodes, elements), jnp.float32),
            pltpu.VMEM((2, rows, elements), jnp.float32),
            pltpu.VMEM((rows, elements), jnp.float32),
            pltpu.VMEM((rows + nodes, elements), jnp.float32),
            pltpu.VMEM((2, members + 1, 2, PLANE - EXTENT, elements), jnp.float32),
            pltpu.VMEM((2, members + 1, 2, PLANE - EXTENT, elements), jnp.float32),
            pltpu.SemaphoreType.DMA((3,)),
            pltpu.SemaphoreType.DMA((2, members + 1, 2)),
            pltpu.SemaphoreType.DMA((2, members + 1, 2)),
        ],
        compiler_params=pltpu.CompilerParams(
            collective_id=0, has_side_effects=True, vmem_limit_bytes=24 * 1024 * 1024
        ),
    )(scalars, transport, mass, element_order, jnp.asarray(split_matrix()))
    block = pl.BlockSpec((nodes // 2, elements), lambda step: (step, 0))
    slots = pl.pallas_call(
        slot_kernel,
        out_shape=jax.ShapeDtypeStruct((rows, elements), jnp.float32),
        grid=(2 * members,),
        in_specs=[pl.BlockSpec(element_order.shape, lambda step: (0, 0)), block],
        out_specs=block,
        compiler_params=pltpu.CompilerParams(vmem_limit_bytes=8 * 1024 * 1024),
    )(element_order, final)
    return slots.reshape(scalars.shape)


def solution(mesh):
    in_specs = (P("ens", None, "elem"), P(None, None, "elem"), P(None, "elem"), P("elem", None))
    out_specs = P("ens", None, "elem")
    return jax.shard_map(
        per_device, mesh=mesh, in_specs=in_specs, out_specs=out_specs, check_vma=False
    )
```
